128 devices in a mesh: row: 8 (over x, z_hi), col: 16 (over y, z_lo, core).
Axes of the slice: x: 4, y: 4, z: 4 (z_hi: 2, z_lo: 2; z = z_hi * 2 + z_lo), core: 2. Of those that a mesh axis runs over, the one named last changes fastest.
Arguments:
- gradients: bfloat16 [3, 128, 512, 512], P(None, None, ('row', 'col')), may hold values from -6 to 6
- factors: float32 [2, 128, 512, 512], P(None, None, ('row', 'col')), as said below
- slot_block: int32 [128], replicated, may hold values from 0 to 127, each once
- layer_of_block: int32 [128], replicated, may hold values from 0 to 3
- layer_step_scale: float32 [4], replicated, may hold values from 0.25 to 4
Outputs:
- new_factors: float32 [2, 128, 512, 512], P(None, ('row', 'col'))
- update: bfloat16 [128, 512, 512], P(None, ('row', 'col'))
The draws below stay inside these ranges and needn't reach their ends.
Inputs may be any that keep to these rules, and one draw needn't show every extreme that they name: Every block factors[i, b] is symmetric positive definite with eigenvalues of 0.25 or more. `slot_block`: each block number stands in exactly one slot; slot j belongs to owner device j in the order of row+col (one slot per device).
All inputs are finite; a program needn't handle non-finite values.
Results may differ from the reference program's by a relative error of at most 0.0069.
Values may be sent and summed in bfloat16 or wider, within the bound.
No kernel may reach another device: no remote copies, remote signals or barrier semaphores. Data moves between devices by JAX's collectives and lax.ppermute only.
A program may use at most 64 MiB of HBM per device.

```python
import math
import jax
import jax.numpy as jnp
from jax import lax

BS = 512
STEPS = 3
ITERS = 6
LAYERS = 4
NB = 128


def draw_factors(key, part):
    key_list = jax.random.split(jax.random.fold_in(key, 7), 2 * NB)

    def single(one_key):
        first_key = jax.random.fold_in(one_key, 1)
        second_key = jax.random.fold_in(one_key, 2)
        mixing = jax.random.normal(first_key, (BS, BS), jnp.float32)
        spread = jnp.exp(jax.random.uniform(second_key, (BS,), jnp.float32, 0.0, math.log(3.0)))
        inner_part = jnp.dot(mixing, mixing.T, precision=lax.Precision.HIGHEST) / BS + 0.25 * jnp.eye(BS, dtype=jnp.float32)
        return inner_part * spread[:, None] * spread[None, :]
    blocks = lax.map(single, key_list)
    return blocks.reshape(2, NB, BS, BS)


def plant(array, rng, least, largest):
    longest = array.shape.index(max(array.shape))
    spots = []
    for shift in (0, 1):
        where = [jax.random.randint(jax.random.fold_in(rng, axis), (), 0, length) for axis, length in enumerate(array.shape)]
        where[longest] = (where[longest] + shift) % array.shape[longest]
        spots.append(tuple(where))
    return array.at[spots[0]].set(least).at[spots[1]].set(largest)


def level_of(rng, dims, pieces, smallest, high):
    factor_of, own = 1.0, jax.random.fold_in(rng, 6)
    for axis_at, shards_of in pieces:
        steps = jnp.exp(jax.random.uniform(jax.random.fold_in(own, axis_at), (shards_of,), jnp.float32, smallest / len(pieces), high / len(pieces)))
        factor_of = factor_of * jnp.repeat(steps, dims[axis_at] // shards_of).reshape([-1 if axis == axis_at else 1 for axis in range(len(dims))])
    return factor_of


def gaussian(key, dims, width, limit, shards=(), kind=jnp.bfloat16):
    factor_of = level_of(key, dims, shards, -0.22, 0.18) if shards else 1.0
    entries = jax.random.normal(key, dims, jnp.float32) * width * factor_of
    return jnp.minimum(jnp.maximum(entries, -limit), limit).astype(kind)


def setup_inputs(seed: int = 0) -> dict:
    key_of = jax.random.split(jax.random.key(seed), 6)
    gradients = gaussian(key_of[0], (STEPS, NB, BS, BS), 1.0, 6.0, ((2, 128),))
    factors = draw_factors(jax.random.fold_in(key_of[5], 71), 0)
    slot_block = jax.random.permutation(key_of[2], NB).astype(jnp.int32)
    layer_of_block = plant(jax.random.randint(key_of[3], (NB,), 0, LAYERS), jax.random.fold_in(key_of[3], 1), 0, LAYERS - 1).astype(jnp.int32)
    layer_step_scale = jnp.clip(jnp.exp(jax.random.uniform(key_of[4], (LAYERS,), jnp.float32, math.log(0.25), math.log(4.0))), 0.25, 4.0)
    return {"gradients": gradients, "factors": factors, "slot_block": slot_block, "layer_of_block": layer_of_block, "layer_step_scale": layer_step_scale}


def inverse_root(matrix):
    unit_matrix = jnp.eye(matrix.shape[0], dtype=jnp.float32)
    frobenius = jnp.sqrt(jnp.sum(matrix * matrix))
    mixer = matrix / frobenius
    approx = unit_matrix * frobenius ** (-0.25)
    for newton_sweep in range(ITERS):
        factor_p = (5.0 * unit_matrix - mixer) * 0.25
        approx = jnp.dot(approx, factor_p, precision=lax.Precision.HIGHEST)
        second_root_factor = jnp.dot(factor_p, factor_p, precision=lax.Precision.HIGHEST)
        mixer = jnp.dot(second_root_factor, jnp.dot(second_root_factor, mixer, precision=lax.Precision.HIGHEST), precision=lax.Precision.HIGHEST)
    return approx

def reference(gradients, factors, slot_block, layer_of_block, layer_step_scale):

    def per_slot(slot):
        block = slot_block[slot]
        gradient = lax.dynamic_index_in_dim(gradients, block, 1, keepdims=False)
        held = lax.dynamic_index_in_dim(factors, block, 1, keepdims=False)
        gram_left = jnp.zeros((BS, BS), jnp.float32)
        gram_right = jnp.zeros((BS, BS), jnp.float32)
        for moment in range(STEPS):
            gram_left = gram_left + jnp.dot(gradient[moment], gradient[moment].T, preferred_element_type=jnp.float32)
            gram_right = gram_right + jnp.dot(gradient[moment].T, gradient[moment], preferred_element_type=jnp.float32)
        left_stat = held[0] + gram_left / BS
        right_stat = held[1] + gram_right / BS
        root_left_half = inverse_root(left_stat).astype(jnp.bfloat16)
        root_right_half = inverse_root(right_stat).astype(jnp.bfloat16)
        step_multiplier = layer_step_scale[layer_of_block[block]]
        left_applied = jnp.dot(root_left_half, gradient[STEPS - 1], preferred_element_type=jnp.float32).astype(jnp.bfloat16)
        product = jnp.dot(left_applied, root_right_half, preferred_element_type=jnp.float32)
        return (left_stat, right_stat, (step_multiplier * product).astype(jnp.bfloat16))
    lefts, rights, moved = lax.map(per_slot, jnp.arange(NB, dtype=jnp.int32))
    new_factors = jnp.stack([lefts, rights])
    update = jnp.zeros_like(moved).at[slot_block].set(moved)
    return (new_factors, update)
```

```python
import jax
import jax.numpy as jnp
from jax import lax
from jax.experimental import pallas as pl
from jax.experimental.pallas import tpu as pltpu
from jax.sharding import PartitionSpec as P

ITERS = 6
TILE = 128
BF = jnp.bfloat16
F32 = jnp.float32


def pack_body(slots, grads, factors, msg, fac_in, fac_out, sem_g, sem_f, sem_o):
    steps, blocks, rows, side = grads.shape
    wide = steps * side
    load = pltpu.make_async_copy(factors, fac_in, sem_f)
    load.start()

    def send(j, carry):
        block = slots[j]
        for s in range(steps):
            pltpu.make_async_copy(
                grads.at[s, block], msg.at[j, :, pl.ds(s * side, side)], sem_g
            ).start()
        return carry

    lax.fori_loop(0, blocks, send, 0, unroll=8)
    load.wait()
    band = lax.axis_index("row") // 2
    tiles = side // TILE
    starts = [pl.multiple_of(lax.rem(band + t, tiles) * TILE, TILE) for t in range(tiles - 1)]

    def convert(j, carry):
        block = slots[j]
        for f in range(2):
            for t in range(tiles - 1):
                piece = fac_in[f, block, :, pl.ds(starts[t], TILE)]
                fac_out[j, :, pl.ds((f * (tiles - 1) + t) * TILE, TILE)] = piece.astype(BF)
        return carry

    lax.fori_loop(0, blocks, convert, 0, unroll=8)
    narrow = fac_out.shape[2]
    store = pltpu.make_async_copy(fac_out, msg.at[:, :, pl.ds(wide, narrow)], sem_o)
    store.start()
    sent = msg.at[:, :, pl.ds(0, wide)]
    pltpu.make_async_copy(sent, sent, sem_g).wait()
    store.wait()


def pack(slots, grads, factors):
    steps, blocks, rows, side = grads.shape
    narrow = 2 * (side - TILE)
    return pl.pallas_call(
        pack_body,
        out_shape=jax.ShapeDtypeStruct((blocks, rows, steps * side + narrow), BF),
        in_specs=[
            pl.BlockSpec(memory_space=pltpu.SMEM),
            pl.BlockSpec(memory_space=pl.ANY),
            pl.BlockSpec(memory_space=pl.ANY),
        ],
        out_specs=pl.BlockSpec(memory_space=pl.ANY),
        scratch_shapes=[
            pltpu.VMEM(factors.shape, F32),
            pltpu.VMEM((blocks, rows, narrow), BF),
            pltpu.SemaphoreType.DMA,
            pltpu.SemaphoreType.DMA,
            pltpu.SemaphoreType.DMA,
        ],
    )(slots, grads, factors)


def mm(a, b):
    return jnp.dot(a, b, preferred_element_type=F32)


def step_of(m):
    mb = m.astype(BF)
    square = mm(mb, mb)
    w = (0.0625 * square - 0.625 * m).astype(BF)
    v = 1.5625 * m + mm(w, mb)
    return 1.5625 * v + mm(w, v.astype(BF))


def compute_body(slots, layers, scales, got, stats, update, stat_ref, m_ref, x_ref, g_ref, sem):
    sources, rows, _ = got.shape
    side = sources * rows
    tiles = side // TILE
    per = sources // tiles
    steps = g_ref.shape[0]
    grams = [None, None]
    for s in range(steps):
        g_ref[s] = got[:, :, s * side : (s + 1) * side].reshape(side, side)
    for s in range(steps):
        g = g_ref[s]
        gt = g.T
        left = mm(g, gt)
        right = mm(gt, g)
        grams = [left, right] if s == 0 else [grams[0] + left, grams[1] + right]
    for f in range(2):
        stat_ref[f, 0] = grams[f] / side
        for i in range(tiles):
            for t in range(tiles - 1):
                k = (i + t) % tiles
                lo = steps * side + (f * (tiles - 1) + t) * TILE
                held = got[i * per : (i + 1) * per, :, lo : lo + TILE]
                held = held.astype(F32).reshape(TILE, TILE)
                a = pl.ds(i * TILE, TILE)
                c = pl.ds(k * TILE, TILE)
                stat_ref[f, 0, a, c] += held
                if t == 1:
                    stat_ref[f, 0, c, a] += held.T
    out = pltpu.make_async_copy(stat_ref, stats, sem)
    out.start()
    eye = (
        lax.broadcasted_iota(jnp.int32, (side, side), 0)
        == lax.broadcasted_iota(jnp.int32, (side, side), 1)
    )
    for f in range(2):
        a = stat_ref[f, 0]
        total = jnp.sum(jnp.sum(a * a, axis=0, keepdims=True), axis=1, keepdims=True)
        norm = jnp.sqrt(total)
        first = lax.rsqrt(jnp.sqrt(norm))
        m = a * (1.0 / norm)
        x_ref[f] = first * (jnp.where(eye, 1.25, 0.0) - 0.25 * m)
        m_ref[f] = step_of(m)

    def sweep(k, carry):
        for f in range(2):
            m = m_ref[f]
            x = x_ref[f]
            x_ref[f] = 1.25 * x - 0.25 * mm(x.astype(BF), m.astype(BF))
            m_ref[f] = step_of(m)
        return carry

    lax.fori_loop(1, ITERS - 1, sweep, 0)
    roots = []
    for f in range(2):
        x = x_ref[f]
        roots.append((1.25 * x - 0.25 * mm(x.astype(BF), m_ref[f].astype(BF))).astype(BF))
    me = lax.axis_index("row") * lax.axis_size("col") + lax.axis_index("col")
    scale = scales[layers[slots[me]]]
    applied = mm(roots[0], g_ref[steps - 1]).astype(BF)
    result = (scale * mm(applied, roots[1])).astype(BF)
    update[...] = result.reshape(sources, rows, side)
    out.wait()


def compute(slots, layers, scales, got, steps):
    sources, rows, _ = got.shape
    side = sources * rows
    smem = pl.BlockSpec(memory_space=pltpu.SMEM)
    return pl.pallas_call(
        compute_body,
        out_shape=(
            jax.ShapeDtypeStruct((2, 1, side, side), F32),
            jax.ShapeDtypeStruct((sources, rows, side), BF),
        ),
        in_specs=[smem, smem, smem, pl.BlockSpec(memory_space=pltpu.VMEM)],
        out_specs=(
            pl.BlockSpec(memory_space=pl.ANY),
            pl.BlockSpec(memory_space=pltpu.VMEM),
        ),
        scratch_shapes=[
            pltpu.VMEM((2, 1, side, side), F32),
            pltpu.VMEM((2, side, side), F32),
            pltpu.VMEM((2, side, side), F32),
            pltpu.VMEM((steps, side, side), BF),
            pltpu.SemaphoreType.DMA,
        ],
    )(slots, layers, scales, got)


def unpack_body(slots, got, update, sem):
    blocks = got.shape[0]

    def place(j, carry):
        pltpu.make_async_copy(got.at[j], update.at[slots[j]], sem).start()
        return carry

    lax.fori_loop(0, blocks, place, 0, unroll=8)
    pltpu.make_async_copy(update, update, sem).wait()


def unpack(slots, got):
    return pl.pallas_call(
        unpack_body,
        out_shape=jax.ShapeDtypeStruct(got.shape, got.dtype),
        in_specs=[
            pl.BlockSpec(memory_space=pltpu.SMEM),
            pl.BlockSpec(memory_space=pl.ANY),
        ],
        out_specs=pl.BlockSpec(memory_space=pl.ANY),
        scratch_shapes=[pltpu.SemaphoreType.DMA],
    )(slots, got)


def body(gradients, factors, slot_block, layer_of_block, layer_step_scale):
    axes = ("row", "col")
    message = pack(slot_block, gradients, factors)
    owned = lax.all_to_all(message, axes, split_axis=0, concat_axis=0, tiled=True)
    new_factors, moved = compute(
        slot_block, layer_of_block, layer_step_scale, owned, gradients.shape[0]
    )
    returned = lax.all_to_all(moved, axes, split_axis=0, concat_axis=0, tiled=True)
    return (new_factors, unpack(slot_block, returned))


def solution(mesh):
    return jax.shard_map(
        body,
        mesh=mesh,
        in_specs=(
            P(None, None, ("row", "col"), None),
            P(None, None, ("row", "col"), None),
            P(),
            P(),
            P(),
        ),
        out_specs=(P(None, ("row", "col"), None, None), P(None, ("row", "col"), None)),
        check_vma=False,
    )
```

```python
import jax
import jax.numpy as jnp
from jax import lax
from jax.experimental import pallas as pl
from jax.experimental.pallas import tpu as pltpu
from jax.sharding import PartitionSpec as P

ITERS = 6
TILE = 128
BF = jnp.bfloat16
F32 = jnp.float32


def pack_body(slots, grads, factors, msg, g_in, f_in, out, sem_g, sem_f, sem_o):
    steps, blocks, rows, side = grads.shape
    wide = steps * side
    tiles = side // TILE
    narrow = (tiles - 1) * TILE
    loads = [pltpu.make_async_copy(grads.at[s], g_in.at[s], sem_g.at[s]) for s in range(steps)]
    loads += [pltpu.make_async_copy(factors.at[f], f_in.at[f], sem_f.at[f]) for f in range(2)]
    for load in loads:
        load.start()
    stores = []

    def flush(lo, size):
        span = pl.ds(lo, size)
        store = pltpu.make_async_copy(
            out.at[:, :, span], msg.at[:, :, span], sem_o.at[len(stores)]
        )
        store.start()
        stores.append(store)

    for s in range(steps):
        loads[s].wait()

        def gather(j, carry):
            out[j, :, pl.ds(s * side, side)] = g_in[s, slots[j]]
            return carry

        lax.fori_loop(0, blocks, gather, 0, unroll=16)
        flush(s * side, side)
    band = lax.axis_index("row") // 2
    starts = [pl.multiple_of(lax.rem(band + t, tiles) * TILE, TILE) for t in range(tiles - 1)]
    for f in range(2):
        loads[steps + f].wait()

        def convert(j, carry):
            block = slots[j]
            for t in range(tiles - 1):
                piece = f_in[f, block, :, pl.ds(starts[t], TILE)]
                out[j, :, pl.ds(wide + f * narrow + t * TILE, TILE)] = piece.astype(BF)
            return carry

        lax.fori_loop(0, blocks, convert, 0, unroll=16)
        flush(wide + f * narrow, narrow)
    for store in stores:
        store.wait()


def pack(slots, grads, factors):
    steps, blocks, rows, side = grads.shape
    shape = (blocks, rows, steps * side + 2 * (side - TILE))
    return pl.pallas_call(
        pack_body,
        out_shape=jax.ShapeDtypeStruct(shape, BF),
        in_specs=[
            pl.BlockSpec(memory_space=pltpu.SMEM),
            pl.BlockSpec(memory_space=pl.ANY),
            pl.BlockSpec(memory_space=pl.ANY),
        ],
        out_specs=pl.BlockSpec(memory_space=pl.ANY),
        scratch_shapes=[
            pltpu.VMEM(grads.shape, BF),
            pltpu.VMEM(factors.shape, F32),
            pltpu.VMEM(shape, BF),
            pltpu.SemaphoreType.DMA((steps,)),
            pltpu.SemaphoreType.DMA((2,)),
            pltpu.SemaphoreType.DMA((steps + 2,)),
        ],
    )(slots, grads, factors)


def mm(a, b):
    return jnp.dot(a, b, preferred_element_type=F32)


def step_of(m):
    mb = m.astype(BF)
    square = mm(mb, mb)
    w = (0.0625 * square - 0.625 * m).astype(BF)
    v = 1.5625 * m + mm(w, mb)
    return 1.5625 * v + mm(w, v.astype(BF))


def compute_body(slots, layers, scales, got, stats, update, stat_ref, m_ref, x_ref, g_ref, sem):
    sources, rows, _ = got.shape
    side = sources * rows
    tiles = side // TILE
    per = sources // tiles
    steps = g_ref.shape[0]
    grams = [None, None]
    for s in range(steps):
        g_ref[s] = got[:, :, s * side : (s + 1) * side].reshape(side, side)
    for s in range(steps):
        g = g_ref[s]
        gt = g.T
        left = mm(g, gt)
        right = mm(gt, g)
        grams = [left, right] if s == 0 else [grams[0] + left, grams[1] + right]
    for f in range(2):
        stat_ref[f, 0] = grams[f] / side
        for i in range(tiles):
            for t in range(tiles - 1):
                k = (i + t) % tiles
                lo = steps * side + (f * (tiles - 1) + t) * TILE
                held = got[i * per : (i + 1) * per, :, lo : lo + TILE]
                held = held.astype(F32).reshape(TILE, TILE)
                a = pl.ds(i * TILE, TILE)
                c = pl.ds(k * TILE, TILE)
                stat_ref[f, 0, a, c] += held
                if t == 1:
                    stat_ref[f, 0, c, a] += held.T
    out = pltpu.make_async_copy(stat_ref, stats, sem)
    out.start()
    eye = (
        lax.broadcasted_iota(jnp.int32, (side, side), 0)
        == lax.broadcasted_iota(jnp.int32, (side, side), 1)
    )
    for f in range(2):
        a = stat_ref[f, 0]
        total = jnp.sum(jnp.sum(a * a, axis=0, keepdims=True), axis=1, keepdims=True)
        norm = jnp.sqrt(total)
        first = lax.rsqrt(jnp.sqrt(norm))
        m = a * (1.0 / norm)
        x_ref[f] = first * (jnp.where(eye, 1.25, 0.0) - 0.25 * m)
        m_ref[f] = step_of(m)

    def sweep(k, carry):
        for f in range(2):
            m = m_ref[f]
            x = x_ref[f]
            x_ref[f] = 1.25 * x - 0.25 * mm(x.astype(BF), m.astype(BF))
            m_ref[f] = step_of(m)
        return carry

    lax.fori_loop(1, ITERS - 1, sweep, 0)
    roots = []
    for f in range(2):
        x = x_ref[f]
        roots.append((1.25 * x - 0.25 * mm(x.astype(BF), m_ref[f].astype(BF))).astype(BF))
    me = lax.axis_index("row") * lax.axis_size("col") + lax.axis_index("col")
    scale = scales[layers[slots[me]]]
    applied = mm(roots[0], g_ref[steps - 1]).astype(BF)
    result = (scale * mm(applied, roots[1])).astype(BF)
    update[...] = result.reshape(sources, rows, side)
    out.wait()


def compute(slots, layers, scales, got, steps):
    sources, rows, _ = got.shape
    side = sources * rows
    smem = pl.BlockSpec(memory_space=pltpu.SMEM)
    return pl.pallas_call(
        compute_body,
        out_shape=(
            jax.ShapeDtypeStruct((2, 1, side, side), F32),
            jax.ShapeDtypeStruct((sources, rows, side), BF),
        ),
        in_specs=[smem, smem, smem, pl.BlockSpec(memory_space=pltpu.VMEM)],
        out_specs=(
            pl.BlockSpec(memory_space=pl.ANY),
            pl.BlockSpec(memory_space=pltpu.VMEM),
        ),
        scratch_shapes=[
            pltpu.VMEM((2, 1, side, side), F32),
            pltpu.VMEM((2, side, side), F32),
            pltpu.VMEM((2, side, side), F32),
            pltpu.VMEM((steps, side, side), BF),
            pltpu.SemaphoreType.DMA,
        ],
    )(slots, layers, scales, got)


def unpack_body(slots, got, update):
    blocks = got.shape[0]

    def place(j, carry):
        update[slots[j]] = got[j]
        return carry

    lax.fori_loop(0, blocks, place, 0, unroll=16)


def unpack(slots, got):
    return pl.pallas_call(
        unpack_body,
        out_shape=jax.ShapeDtypeStruct(got.shape, got.dtype),
        in_specs=[
            pl.BlockSpec(memory_space=pltpu.SMEM),
            pl.BlockSpec(memory_space=pltpu.VMEM),
        ],
        out_specs=pl.BlockSpec(memory_space=pltpu.VMEM),
    )(slots, got)


def body(gradients, factors, slot_block, layer_of_block, layer_step_scale):
    axes = ("row", "col")
    message = pack(slot_block, gradients, factors)
    owned = lax.all_to_all(message, axes, split_axis=0, concat_axis=0, tiled=True)
    new_factors, moved = compute(
        slot_block, layer_of_block, layer_step_scale, owned, gradients.shape[0]
    )
    returned = lax.all_to_all(moved, axes, split_axis=0, concat_axis=0, tiled=True)
    return (new_factors, unpack(slot_block, returned))


def solution(mesh):
    return jax.shard_map(
        body,
        mesh=mesh,
        in_specs=(
            P(None, None, ("row", "col"), None),
            P(None, None, ("row", "col"), None),
            P(),
            P(),
            P(),
        ),
        out_specs=(P(None, ("row", "col"), None, None), P(None, ("row", "col"), None)),
        check_vma=False,
    )
```

```python
import jax
import jax.numpy as jnp
from jax import lax
from jax.experimental import pallas as pl
from jax.experimental.pallas import tpu as pltpu
from jax.sharding import PartitionSpec as P

ITERS = 6
TILE = 128
BF = jnp.bfloat16
F32 = jnp.float32


def pack_body(slots, grads, factors, msg, g_in, f_in, sem_g, sem_f):
    steps, blocks, rows, side = grads.shape
    wide = steps * side
    tiles = side // TILE
    narrow = (tiles - 1) * TILE
    loads = [pltpu.make_async_copy(grads.at[s], g_in.at[s], sem_g.at[s]) for s in range(steps)]
    loads += [pltpu.make_async_copy(factors.at[f], f_in.at[f], sem_f.at[f]) for f in range(2)]
    for load in loads:
        load.start()
    for s in range(steps):
        loads[s].wait()

        def gather(j, carry):
            msg[j, :, pl.ds(s * side, side)] = g_in[s, slots[j]]
            return carry

        lax.fori_loop(0, blocks, gather, 0, unroll=16)
    band = lax.axis_index("row") // 2
    starts = [pl.multiple_of(lax.rem(band + t, tiles) * TILE, TILE) for t in range(tiles - 1)]
    for f in range(2):
        loads[steps + f].wait()

        def convert(j, carry):
            block = slots[j]
            for t in range(tiles - 1):
                piece = f_in[f, block, :, pl.ds(starts[t], TILE)]
                msg[j, :, pl.ds(wide + f * narrow + t * TILE, TILE)] = piece.astype(BF)
            return carry

        lax.fori_loop(0, blocks, convert, 0, unroll=16)


def pack(slots, grads, factors):
    steps, blocks, rows, side = grads.shape
    shape = (blocks, rows, steps * side + 2 * (side - TILE))
    return pl.pallas_call(
        pack_body,
        out_shape=pltpu.VMEM(shape, BF),
        in_specs=[
            pl.BlockSpec(memory_space=pltpu.SMEM),
            pl.BlockSpec(memory_space=pl.ANY),
            pl.BlockSpec(memory_space=pl.ANY),
        ],
        out_specs=pl.BlockSpec(memory_space=pltpu.VMEM),
        scratch_shapes=[
            pltpu.VMEM(grads.shape, BF),
            pltpu.VMEM(factors.shape, F32),
            pltpu.SemaphoreType.DMA((steps,)),
            pltpu.SemaphoreType.DMA((2,)),
        ],
    )(slots, grads, factors)


def mm(a, b):
    return jnp.dot(a, b, preferred_element_type=F32)


def put(ref, f, top, low):
    half = low.shape[0]
    ref[f, :half, :] = top
    ref[f, half:, :half] = top[:, half:].T
    ref[f, half:, half:] = low


def symmetric_product(a_ref, b_ref, f):
    half = a_ref.shape[1] // 2
    top = mm(a_ref[f, :half, :], b_ref[f])
    low = mm(a_ref[f, half:, :], b_ref[f, :, half:])
    return top, low


def compute_body(
    slots, layers, scales, got, stats, update,
    raw, held, stat_ref, top_ref, low_ref, m_ref, x_ref, w_ref, g_ref, t_ref, sem, sem_in,
):
    sources, rows, _ = got.shape
    side = sources * rows
    half = side // 2
    tiles = side // TILE
    per = sources // tiles
    steps = g_ref.shape[0]
    loads = [
        pltpu.make_async_copy(got.at[:, :, pl.ds(s * side, side)], raw.at[s], sem_in.at[s])
        for s in range(steps)
    ]
    rest = pl.ds(steps * side, held.shape[2])
    loads.append(pltpu.make_async_copy(got.at[:, :, rest], held, sem_in.at[steps]))
    for load in loads:
        load.start()
    grams = [None, None]
    for s in range(steps):
        loads[s].wait()
        g_ref[s] = raw[s].reshape(side, side)
        t_ref[s] = g_ref[s].T
        pairs = ((g_ref, t_ref), (t_ref, g_ref))
        for f, (left, right) in enumerate(pairs):
            new = symmetric_product(left, right, s)
            grams[f] = new if s == 0 else tuple(a + b for a, b in zip(grams[f], new))
    loads[steps].wait()

    def block(f, i, t):
        lo = (f * (tiles - 1) + t) * TILE
        piece = held[i * per : (i + 1) * per, :, lo : lo + TILE]
        return piece.reshape(TILE, TILE).astype(F32)

    mid = tiles // 2
    for f in range(2):
        stat_ref[f, 0, :half, :] = grams[f][0] / side
        stat_ref[f, 0, half:, half:] = grams[f][1] / side
        for i in range(tiles):
            for k in range(tiles):
                if i >= mid and k < mid:
                    continue
                t = (k - i) % tiles
                piece = block(f, i, t) if t < tiles - 1 else block(f, k, 1).T
                a = slice(i * TILE, (i + 1) * TILE)
                c = slice(k * TILE, (k + 1) * TILE)
                stat_ref[f, 0, a, c] += piece
        stat_ref[f, 0, half:, :half] = stat_ref[f, 0, :half, half:].T
    out = pltpu.make_async_copy(stat_ref, stats, sem)
    out.start()
    eye = (
        lax.broadcasted_iota(jnp.int32, (half, half), 0)
        == lax.broadcasted_iota(jnp.int32, (half, half), 1)
    )
    unit = jnp.where(eye, 1.25, 0.0)
    wide_unit = jnp.concatenate([unit, jnp.zeros((half, half), F32)], axis=1)

    def total(x):
        return jnp.sum(jnp.sum(x * x, axis=0, keepdims=True), axis=1, keepdims=True)

    for f in range(2):
        top = stat_ref[f, 0, :half, :]
        low = stat_ref[f, 0, half:, half:]
        square = total(top) + total(top[:, half:]) + total(low)
        norm = jnp.sqrt(square)
        first = lax.rsqrt(jnp.sqrt(norm))
        top = top * (1.0 / norm)
        low = low * (1.0 / norm)
        top_ref[0, f] = top
        low_ref[0, f] = low
        put(m_ref, f, top.astype(BF), low.astype(BF))
        top = first * (wide_unit - 0.25 * top)
        low = first * (unit - 0.25 * low)
        top_ref[1, f] = top
        low_ref[1, f] = low
        put(x_ref, f, top.astype(BF), low.astype(BF))

    def move_x(f):
        top, low = symmetric_product(x_ref, m_ref, f)
        top = 1.25 * top_ref[1, f] - 0.25 * top
        low = 1.25 * low_ref[1, f] - 0.25 * low
        top_ref[1, f] = top
        low_ref[1, f] = low
        put(x_ref, f, top.astype(BF), low.astype(BF))

    def move_m():
        for f in range(2):
            top, low = symmetric_product(m_ref, m_ref, f)
            top = 0.0625 * top - 0.625 * top_ref[0, f]
            low = 0.0625 * low - 0.625 * low_ref[0, f]
            put(w_ref, f, top.astype(BF), low.astype(BF))
        for f in range(2):
            top, low = symmetric_product(w_ref, m_ref, f)
            top = 1.5625 * top_ref[0, f] + top
            low = 1.5625 * low_ref[0, f] + low
            top_ref[0, f] = top
            low_ref[0, f] = low
            put(m_ref, f, top.astype(BF), low.astype(BF))
        for f in range(2):
            top, low = symmetric_product(w_ref, m_ref, f)
            top = 1.5625 * top_ref[0, f] + top
            low = 1.5625 * low_ref[0, f] + low
            top_ref[0, f] = top
            low_ref[0, f] = low
            put(m_ref, f, top.astype(BF), low.astype(BF))

    move_m()

    def sweep(k, carry):
        for f in range(2):
            move_x(f)
        move_m()
        return carry

    lax.fori_loop(1, ITERS - 1, sweep, 0)
    for f in range(2):
        move_x(f)
    me = lax.axis_index("row") * lax.axis_size("col") + lax.axis_index("col")
    scale = scales[layers[slots[me]]]
    applied = mm(x_ref[0], g_ref[steps - 1]).astype(BF)
    result = (scale * mm(applied, x_ref[1])).astype(BF)
    update[...] = result.reshape(sources, rows, side)
    out.wait()


def compute(slots, layers, scales, got, steps):
    sources, rows, wide = got.shape
    side = sources * rows
    half = side // 2
    smem = pl.BlockSpec(memory_space=pltpu.SMEM)
    return pl.pallas_call(
        compute_body,
        out_shape=(
            jax.ShapeDtypeStruct((2, 1, side, side), F32),
            pltpu.VMEM((sources, rows, side), BF),
        ),
        in_specs=[smem, smem, smem, pl.BlockSpec(memory_space=pl.ANY)],
        out_specs=(
            pl.BlockSpec(memory_space=pl.ANY),
            pl.BlockSpec(memory_space=pltpu.VMEM),
        ),
        scratch_shapes=[
            pltpu.VMEM((steps, sources, rows, side), BF),
            pltpu.VMEM((sources, rows, wide - steps * side), BF),
            pltpu.VMEM((2, 1, side, side), F32),
            pltpu.VMEM((2, 2, half, side), F32),
            pltpu.VMEM((2, 2, half, half), F32),
            pltpu.VMEM((2, side, side), BF),
            pltpu.VMEM((2, side, side), BF),
            pltpu.VMEM((2, side, side), BF),
            pltpu.VMEM((steps, side, side), BF),
            pltpu.VMEM((steps, side, side), BF),
            pltpu.SemaphoreType.DMA,
            pltpu.SemaphoreType.DMA((steps + 1,)),
        ],
    )(slots, layers, scales, got)


def unpack_body(slots, got, update):
    blocks = got.shape[0]

    def place(j, carry):
        update[slots[j]] = got[j]
        return carry

    lax.fori_loop(0, blocks, place, 0, unroll=16)


def unpack(slots, got):
    return pl.pallas_call(
        unpack_body,
        out_shape=jax.ShapeDtypeStruct(got.shape, got.dtype),
        in_specs=[
            pl.BlockSpec(memory_space=pltpu.SMEM),
            pl.BlockSpec(memory_space=pltpu.VMEM),
        ],
        out_specs=pl.BlockSpec(memory_space=pltpu.VMEM),
    )(slots, got)


def body(gradients, factors, slot_block, layer_of_block, layer_step_scale):
    axes = ("row", "col")
    message = pack(slot_block, gradients, factors)
    owned = lax.all_to_all(message, axes, split_axis=0, concat_axis=0, tiled=True)
    new_factors, moved = compute(
        slot_block, layer_of_block, layer_step_scale, owned, gradients.shape[0]
    )
    returned = lax.all_to_all(moved, axes, split_axis=0, concat_axis=0, tiled=True)
    returned = pltpu.with_memory_space_constraint(returned, pltpu.VMEM)
    return (new_factors, unpack(slot_block, returned))


def solution(mesh):
    return jax.shard_map(
        body,
        mesh=mesh,
        in_specs=(
            P(None, None, ("row", "col"), None),
            P(None, None, ("row", "col"), None),
            P(),
            P(),
            P(),
        ),
        out_specs=(P(None, ("row", "col"), None, None), P(None, ("row", "col"), None)),
        check_vma=False,
    )
```

```python
import jax
import jax.numpy as jnp
from jax import lax
from jax.experimental import pallas as pl
from jax.experimental.pallas import tpu as pltpu
from jax.sharding import PartitionSpec as P

ITERS = 6
TILE = 128
LIMIT = 32 * 1024 * 1024
BF = jnp.bfloat16
F32 = jnp.float32


def pack_body(slots, grads, factors, msg, g_in, f_in, sem_g, sem_f):
    steps, blocks, rows, side = grads.shape
    wide = steps * side
    tiles = side // TILE
    narrow = (tiles - 1) * TILE
    loads = [pltpu.make_async_copy(grads.at[s], g_in.at[s], sem_g.at[s]) for s in range(steps)]
    loads += [pltpu.make_async_copy(factors.at[f], f_in.at[f], sem_f.at[f]) for f in range(2)]
    for load in loads:
        load.start()
    for s in range(steps):
        loads[s].wait()

        def gather(j, carry):
            msg[j, :, pl.ds(s * side, side)] = g_in[s, slots[j]]
            return carry

        lax.fori_loop(0, blocks, gather, 0, unroll=16)
    band = lax.axis_index("row") // 2
    starts = [pl.multiple_of(lax.rem(band + t, tiles) * TILE, TILE) for t in range(tiles - 1)]
    for f in range(2):
        loads[steps + f].wait()

        def convert(j, carry):
            block = slots[j]
            for t in range(tiles - 1):
                piece = f_in[f, block, :, pl.ds(starts[t], TILE)]
                msg[j, :, pl.ds(wide + f * narrow + t * TILE, TILE)] = piece.astype(BF)
            return carry

        lax.fori_loop(0, blocks, convert, 0, unroll=16)


def pack(slots, grads, factors):
    steps, blocks, rows, side = grads.shape
    shape = (blocks, rows, steps * side + 2 * (side - TILE))
    return pl.pallas_call(
        pack_body,
        out_shape=pltpu.VMEM(shape, BF),
        in_specs=[
            pl.BlockSpec(memory_space=pltpu.SMEM),
            pl.BlockSpec(memory_space=pl.ANY),
            pl.BlockSpec(memory_space=pl.ANY),
        ],
        out_specs=pl.BlockSpec(memory_space=pltpu.VMEM),
        scratch_shapes=[
            pltpu.VMEM(grads.shape, BF),
            pltpu.VMEM(factors.shape, F32),
            pltpu.SemaphoreType.DMA((steps,)),
            pltpu.SemaphoreType.DMA((2,)),
        ],
        compiler_params=pltpu.CompilerParams(vmem_limit_bytes=LIMIT),
    )(slots, grads, factors)


def mm(a, b):
    return jnp.dot(a, b, preferred_element_type=F32)


def put(ref, f, top, low):
    half = low.shape[0]
    ref[f, :half, :] = top
    ref[f, half:, :half] = top[:, half:].T
    ref[f, half:, half:] = low


def symmetric_product(a_ref, b_ref, f):
    half = a_ref.shape[1] // 2
    top = mm(a_ref[f, :half, :], b_ref[f])
    low = mm(a_ref[f, half:, :], b_ref[f, :, half:])
    return top, low


def compute_body(
    slots, layers, scales, got, stats, update,
    stat_ref, top_ref, low_ref, m_ref, x_ref, w_ref, g_ref, t_ref, sem,
):
    sources, rows, _ = got.shape
    side = sources * rows
    half = side // 2
    tiles = side // TILE
    per = sources // tiles
    steps = g_ref.shape[0]
    mid = tiles // 2

    def block(f, i, t):
        lo = steps * side + (f * (tiles - 1) + t) * TILE
        piece = got[i * per : (i + 1) * per, :, lo : lo + TILE]
        return piece.reshape(TILE, TILE).astype(F32)

    for s in range(steps):
        g_ref[s] = got[:, :, s * side : (s + 1) * side].reshape(side, side)
        t_ref[s] = g_ref[s].T
    for f, (left, right) in enumerate(((g_ref, t_ref), (t_ref, g_ref))):
        parts = [symmetric_product(left, right, s) for s in range(steps)]
        top = sum(part[0] for part in parts[1:]) + parts[0][0]
        low = sum(part[1] for part in parts[1:]) + parts[0][1]
        for i in range(tiles):
            for k in range(tiles):
                if i >= mid and k < mid:
                    continue
                t = (k - i) % tiles
                piece = block(f, i, t) if t < tiles - 1 else block(f, k, 1).T
                a = slice(i * TILE, (i + 1) * TILE)
                c = slice(k * TILE, (k + 1) * TILE)
                if i < mid:
                    gram = top[a, c]
                else:
                    gram = low[(i - mid) * TILE : (i - mid + 1) * TILE, (k - mid) * TILE : (k - mid + 1) * TILE]
                stat_ref[f, 0, a, c] = gram * (1.0 / side) + piece
        put(m_ref, f, stat_ref[f, 0, :half, :].astype(BF), stat_ref[f, 0, half:, half:].astype(BF))
        stat_ref[f, 0, half:, :half] = stat_ref[f, 0, :half, half:].T
    out = pltpu.make_async_copy(stat_ref, stats, sem)
    out.start()
    eye = (
        lax.broadcasted_iota(jnp.int32, (half, half), 0)
        == lax.broadcasted_iota(jnp.int32, (half, half), 1)
    )
    unit = jnp.where(eye, 1.25, 0.0)
    wide_unit = jnp.concatenate([unit, jnp.zeros((half, half), F32)], axis=1)

    def total(x):
        return jnp.sum(jnp.sum(x * x, axis=0, keepdims=True), axis=1, keepdims=True)

    inverse = []
    for f in range(2):
        top = stat_ref[f, 0, :half, :]
        low = stat_ref[f, 0, half:, half:]
        norm = jnp.sqrt(total(top) + total(top[:, half:]) + total(low))
        inverse.append((1.0 / norm, lax.rsqrt(jnp.sqrt(norm))))
    for f in range(2):
        inv = inverse[f][0]
        top, low = symmetric_product(m_ref, m_ref, f)
        top = (0.0625 * top * inv - 0.625 * stat_ref[f, 0, :half, :]) * inv
        low = (0.0625 * low * inv - 0.625 * stat_ref[f, 0, half:, half:]) * inv
        put(w_ref, f, top.astype(BF), low.astype(BF))
    for f in range(2):
        inv, first = inverse[f]
        stat_top = stat_ref[f, 0, :half, :]
        stat_low = stat_ref[f, 0, half:, half:]
        top, low = symmetric_product(w_ref, m_ref, f)
        top = (1.5625 * stat_top + top) * inv
        low = (1.5625 * stat_low + low) * inv
        top_ref[0, f] = top
        low_ref[0, f] = low
        put(m_ref, f, top.astype(BF), low.astype(BF))
        top = first * (wide_unit - (0.25 * inv) * stat_top)
        low = first * (unit - (0.25 * inv) * stat_low)
        top_ref[1, f] = top
        low_ref[1, f] = low
        put(x_ref, f, top.astype(BF), low.astype(BF))

    def last_m():
        for f in range(2):
            top, low = symmetric_product(w_ref, m_ref, f)
            top = 1.5625 * top_ref[0, f] + top
            low = 1.5625 * low_ref[0, f] + low
            top_ref[0, f] = top
            low_ref[0, f] = low
            put(m_ref, f, top.astype(BF), low.astype(BF))

    last_m()

    def move_x(f):
        top, low = symmetric_product(x_ref, m_ref, f)
        top = 1.25 * top_ref[1, f] - 0.25 * top
        low = 1.25 * low_ref[1, f] - 0.25 * low
        top_ref[1, f] = top
        low_ref[1, f] = low
        put(x_ref, f, top.astype(BF), low.astype(BF))

    def move_m():
        for f in range(2):
            top, low = symmetric_product(m_ref, m_ref, f)
            top = 0.0625 * top - 0.625 * top_ref[0, f]
            low = 0.0625 * low - 0.625 * low_ref[0, f]
            put(w_ref, f, top.astype(BF), low.astype(BF))
        last_m()
        last_m()

    def sweep(k, carry):
        for f in range(2):
            move_x(f)
        move_m()
        return carry

    lax.fori_loop(1, ITERS - 1, sweep, 0)
    for f in range(2):
        move_x(f)
    me = lax.axis_index("row") * lax.axis_size("col") + lax.axis_index("col")
    scale = scales[layers[slots[me]]]
    applied = mm(x_ref[0], g_ref[steps - 1]).astype(BF)
    result = (scale * mm(applied, x_ref[1])).astype(BF)
    update[...] = result.reshape(sources, rows, side)
    out.wait()


def compute(slots, layers, scales, got, steps):
    sources, rows, _ = got.shape
    side = sources * rows
    half = side // 2
    smem = pl.BlockSpec(memory_space=pltpu.SMEM)
    return pl.pallas_call(
        compute_body,
        out_shape=(
            jax.ShapeDtypeStruct((2, 1, side, side), F32),
            pltpu.VMEM((sources, rows, side), BF),
        ),
        in_specs=[smem, smem, smem, pl.BlockSpec(memory_space=pltpu.VMEM)],
        out_specs=(
            pl.BlockSpec(memory_space=pl.ANY),
            pl.BlockSpec(memory_space=pltpu.VMEM),
        ),
        scratch_shapes=[
            pltpu.VMEM((2, 1, side, side), F32),
            pltpu.VMEM((2, 2, half, side), F32),
            pltpu.VMEM((2, 2, half, half), F32),
            pltpu.VMEM((2, side, side), BF),
            pltpu.VMEM((2, side, side), BF),
            pltpu.VMEM((2, side, side), BF),
            pltpu.VMEM((steps, side, side), BF),
            pltpu.VMEM((steps, side, side), BF),
            pltpu.SemaphoreType.DMA,
        ],
        compiler_params=pltpu.CompilerParams(vmem_limit_bytes=LIMIT),
    )(slots, layers, scales, got)


def unpack_body(slots, got, update):
    blocks = got.shape[0]

    def place(j, carry):
        update[slots[j]] = got[j]
        return carry

    lax.fori_loop(0, blocks, place, 0, unroll=16)


def unpack(slots, got):
    return pl.pallas_call(
        unpack_body,
        out_shape=jax.ShapeDtypeStruct(got.shape, got.dtype),
        in_specs=[
            pl.BlockSpec(memory_space=pltpu.SMEM),
            pl.BlockSpec(memory_space=pltpu.VMEM),
        ],
        out_specs=pl.BlockSpec(memory_space=pltpu.VMEM),
        compiler_params=pltpu.CompilerParams(vmem_limit_bytes=LIMIT),
    )(slots, got)


def in_hbm(x):
    return pltpu.with_memory_space_constraint(x, pltpu.HBM)


def body(gradients, factors, slot_block, layer_of_block, layer_step_scale):
    axes = ("row", "col")
    tables = (slot_block, layer_of_block, layer_step_scale)
    slot_block, layer_of_block, layer_step_scale = map(in_hbm, tables)
    gradients = in_hbm(gradients)
    factors = in_hbm(factors)
    message = pack(slot_block, gradients, factors)
    owned = lax.all_to_all(message, axes, split_axis=0, concat_axis=0, tiled=True)
    owned = pltpu.with_memory_space_constraint(owned, pltpu.VMEM)
    new_factors, moved = compute(
        slot_block, layer_of_block, layer_step_scale, owned, gradients.shape[0]
    )
    returned = lax.all_to_all(moved, axes, split_axis=0, concat_axis=0, tiled=True)
    returned = pltpu.with_memory_space_constraint(returned, pltpu.VMEM)
    return (new_factors, unpack(slot_block, returned))


def solution(mesh):
    return jax.shard_map(
        body,
        mesh=mesh,
        in_specs=(
            P(None, None, ("row", "col"), None),
            P(None, None, ("row", "col"), None),
            P(),
            P(),
            P(),
        ),
        out_specs=(P(None, ("row", "col"), None, None), P(None, ("row", "col"), None)),
        check_vma=False,
    )
```

```python
import jax
import jax.numpy as jnp
from jax import lax
from jax.experimental import pallas as pl
from jax.experimental.pallas import tpu as pltpu
from jax.sharding import PartitionSpec as P

ITERS = 6
TILE = 128
CHUNKS = 4
LIMIT = 32 * 1024 * 1024
BF = jnp.bfloat16
F32 = jnp.float32


def pack_body(
    slots_hbm, grads, factors, msg, places, slots, g_in, f_in, sem_s, sem_g, sem_f
):
    steps, blocks, rows, side = grads.shape
    wide = steps * side
    tiles = side // TILE
    table = pltpu.make_async_copy(slots_hbm, slots, sem_s)
    table.start()
    band = lax.axis_index("row")
    odd = lax.rem(band, 2)
    picks = (2 * odd, 1, 2 - 2 * odd)
    tile_loads = []
    for f in range(2):
        for t, pick in enumerate(picks):
            start = pl.multiple_of(lax.rem(band // 2 + pick, tiles) * TILE, TILE)
            tile = factors.at[f, :, :, pl.ds(start, TILE)]
            tile_loads.append(pltpu.make_async_copy(tile, f_in.at[f, t], sem_f.at[f, t]))
    loads = [pltpu.make_async_copy(grads.at[s], g_in.at[s], sem_g.at[s]) for s in range(steps)]
    for load in loads + tile_loads:
        load.start()
    table.wait()

    def invert(j, carry):
        places[slots[j]] = j
        return carry

    lax.fori_loop(0, blocks, invert, 0, unroll=16)
    for s in range(steps):
        loads[s].wait()

        def gather(j, carry):
            msg[j, :, pl.ds(s * side, side)] = g_in[s, slots[j]]
            return carry

        lax.fori_loop(0, blocks, gather, 0, unroll=16)
    for load in tile_loads:
        load.wait()
    lane = lax.broadcasted_iota(jnp.int32, (rows, TILE), 1)
    mine = (lane // (TILE // 2)) == odd

    def convert(j, carry):
        block = slots[j]
        for f in range(2):
            for t in range(2):
                lo = wide + (2 * f + t) * TILE
                msg[j, :, pl.ds(lo, TILE)] = f_in[f, t, block].astype(BF)
        other = pltpu.roll(f_in[1, 2, block], TILE // 2, 1)
        shared = jnp.where(mine, f_in[0, 2, block], other)
        msg[j, :, pl.ds(wide + 4 * TILE, TILE)] = shared.astype(BF)
        return carry

    lax.fori_loop(0, blocks, convert, 0, unroll=16)


def pack(slots, grads, factors):
    steps, blocks, rows, side = grads.shape
    shape = (blocks, rows, steps * side + 5 * TILE)
    anywhere = pl.BlockSpec(memory_space=pl.ANY)
    return pl.pallas_call(
        pack_body,
        out_shape=(
            pltpu.VMEM(shape, BF),
            jax.ShapeDtypeStruct(slots.shape, jnp.int32),
        ),
        in_specs=[anywhere, anywhere, anywhere],
        out_specs=(
            pl.BlockSpec(memory_space=pltpu.VMEM),
            pl.BlockSpec(memory_space=pltpu.SMEM),
        ),
        scratch_shapes=[
            pltpu.SMEM(slots.shape, jnp.int32),
            pltpu.VMEM(grads.shape, BF),
            pltpu.VMEM((2, 3, blocks, rows, TILE), F32),
            pltpu.SemaphoreType.DMA,
            pltpu.SemaphoreType.DMA((steps,)),
            pltpu.SemaphoreType.DMA((2, 3)),
        ],
        compiler_params=pltpu.CompilerParams(vmem_limit_bytes=LIMIT),
    )(slots, grads, factors)


def mm(a, b):
    return jnp.dot(a, b, preferred_element_type=F32)


def put(ref, f, top, low):
    half = low.shape[0]
    ref[f, :half, :] = top
    ref[f, half:, :half] = top[:, half:].T
    ref[f, half:, half:] = low


def symmetric_product(a_ref, b_ref, f):
    half = a_ref.shape[1] // 2
    right = mm(a_ref[f], b_ref[f, :, half:])
    left = mm(a_ref[f, :half, :], b_ref[f, :, :half])
    return jnp.concatenate([left, right[:half]], axis=1), right[half:]


def compute_body(
    slots, layers, scales, got, stats, update,
    stat_ref, top_ref, low_ref, m_ref, x_ref, w_ref, g_ref, t_ref, sem,
):
    sources, rows, _ = got.shape
    side = sources * rows
    half = side // 2
    tiles = side // TILE
    per = sources // tiles
    steps = g_ref.shape[0]
    mid = tiles // 2

    band = per // 2
    base = steps * side

    def rows_of(i, parity, lo):
        first = i * per + parity * band
        piece = got[first : first + band, :, base + lo : base + lo + TILE]
        return piece.reshape(TILE // 2, TILE).astype(F32)

    def halves(f, i, parity):
        piece = rows_of(i, parity, 4 * TILE)
        return pltpu.roll(piece, TILE // 2, 1) if f else piece

    def own(f, i, parity, t):
        return rows_of(i, parity, (2 * f + t) * TILE)

    def near(f, i):
        return jnp.concatenate([own(f, i, 0, 0), halves(f, i, 1)], axis=0)

    def next_to(f, i):
        return jnp.concatenate([own(f, i, 0, 1), own(f, i, 1, 1)], axis=0)

    def far(f, i):
        return jnp.concatenate([halves(f, i, 0), own(f, i, 1, 0)], axis=0)

    upper_row = lax.broadcasted_iota(jnp.int32, (TILE, TILE), 0) < TILE // 2
    upper_col = lax.broadcasted_iota(jnp.int32, (TILE, TILE), 1) < TILE // 2

    def block(f, i, k):
        t = (k - i) % tiles
        if t == 0:
            piece = near(f, i)
            return jnp.where(jnp.logical_or(upper_row, ~upper_col), piece, piece.T)
        if t == 1:
            return next_to(f, i)
        if t == 2:
            return jnp.where(jnp.logical_or(~upper_row, upper_col), far(f, i), far(f, k).T)
        return next_to(f, k).T

    for s in range(steps):
        g_ref[s] = got[:, :, s * side : (s + 1) * side].reshape(side, side)
        t_ref[s] = g_ref[s].T
    for f, (left, right) in enumerate(((g_ref, t_ref), (t_ref, g_ref))):
        parts = [symmetric_product(left, right, s) for s in range(steps)]
        top = sum(part[0] for part in parts[1:]) + parts[0][0]
        low = sum(part[1] for part in parts[1:]) + parts[0][1]
        for i in range(tiles):
            for k in range(tiles):
                if i >= mid and k < mid:
                    continue
                piece = block(f, i, k)
                a = slice(i * TILE, (i + 1) * TILE)
                c = slice(k * TILE, (k + 1) * TILE)
                if i < mid:
                    gram = top[a, c]
                else:
                    gram = low[(i - mid) * TILE : (i - mid + 1) * TILE, (k - mid) * TILE : (k - mid + 1) * TILE]
                stat_ref[f, 0, a, c] = gram * (1.0 / side) + piece
        put(m_ref, f, stat_ref[f, 0, :half, :].astype(BF), stat_ref[f, 0, half:, half:].astype(BF))
        stat_ref[f, 0, half:, :half] = stat_ref[f, 0, :half, half:].T
    out = pltpu.make_async_copy(stat_ref, stats, sem)
    out.start()
    eye = (
        lax.broadcasted_iota(jnp.int32, (half, half), 0)
        == lax.broadcasted_iota(jnp.int32, (half, half), 1)
    )
    unit = jnp.where(eye, 1.25, 0.0)
    wide_unit = jnp.concatenate([unit, jnp.zeros((half, half), F32)], axis=1)

    def total(x):
        return jnp.sum(jnp.sum(x * x, axis=0, keepdims=True), axis=1, keepdims=True)

    inverse = []
    for f in range(2):
        top = stat_ref[f, 0, :half, :]
        low = stat_ref[f, 0, half:, half:]
        norm = jnp.sqrt(total(top) + total(top[:, half:]) + total(low))
        inverse.append((1.0 / norm, lax.rsqrt(jnp.sqrt(norm))))
    for f in range(2):
        inv = inverse[f][0]
        top, low = symmetric_product(m_ref, m_ref, f)
        top = (0.0625 * top * inv - 0.625 * stat_ref[f, 0, :half, :]) * inv
        low = (0.0625 * low * inv - 0.625 * stat_ref[f, 0, half:, half:]) * inv
        put(w_ref, f, top.astype(BF), low.astype(BF))
    for f in range(2):
        inv, first = inverse[f]
        stat_top = stat_ref[f, 0, :half, :]
        stat_low = stat_ref[f, 0, half:, half:]
        top, low = symmetric_product(w_ref, m_ref, f)
        top = (1.5625 * stat_top + top) * inv
        low = (1.5625 * stat_low + low) * inv
        top_ref[0, f] = top
        low_ref[0, f] = low
        put(m_ref, f, top.astype(BF), low.astype(BF))
        top = first * (wide_unit - (0.25 * inv) * stat_top)
        low = first * (unit - (0.25 * inv) * stat_low)
        top_ref[1, f] = top
        low_ref[1, f] = low
        put(x_ref, f, top.astype(BF), low.astype(BF))

    def last_m():
        for f in range(2):
            top, low = symmetric_product(w_ref, m_ref, f)
            top = 1.5625 * top_ref[0, f] + top
            low = 1.5625 * low_ref[0, f] + low
            top_ref[0, f] = top
            low_ref[0, f] = low
            put(m_ref, f, top.astype(BF), low.astype(BF))

    last_m()

    def move_x(f):
        top, low = symmetric_product(x_ref, m_ref, f)
        top = 1.25 * top_ref[1, f] - 0.25 * top
        low = 1.25 * low_ref[1, f] - 0.25 * low
        top_ref[1, f] = top
        low_ref[1, f] = low
        put(x_ref, f, top.astype(BF), low.astype(BF))

    def move_m():
        for f in range(2):
            top, low = symmetric_product(m_ref, m_ref, f)
            top = 0.0625 * top - 0.625 * top_ref[0, f]
            low = 0.0625 * low - 0.625 * low_ref[0, f]
            put(w_ref, f, top.astype(BF), low.astype(BF))
        last_m()
        last_m()

    def sweep(k, carry):
        for f in range(2):
            move_x(f)
        move_m()
        return carry

    lax.fori_loop(1, ITERS - 1, sweep, 0)
    for f in range(2):
        move_x(f)
    me = lax.axis_index("row") * lax.axis_size("col") + lax.axis_index("col")
    scale = scales[layers[slots[me]]]
    applied = mm(x_ref[0], g_ref[steps - 1]).astype(BF)
    result = (scale * mm(applied, x_ref[1])).astype(BF)
    update[...] = result.reshape(sources, rows, side)
    out.wait()


def compute(slots, layers, scales, got, steps):
    sources, rows, _ = got.shape
    side = sources * rows
    half = side // 2
    smem = pl.BlockSpec(memory_space=pltpu.SMEM)
    return pl.pallas_call(
        compute_body,
        out_shape=(
            jax.ShapeDtypeStruct((2, 1, side, side), F32),
            pltpu.VMEM((sources, rows, side), BF),
        ),
        in_specs=[smem, smem, smem, pl.BlockSpec(memory_space=pltpu.VMEM)],
        out_specs=(
            pl.BlockSpec(memory_space=pl.ANY),
            pl.BlockSpec(memory_space=pltpu.VMEM),
        ),
        scratch_shapes=[
            pltpu.VMEM((2, 1, side, side), F32),
            pltpu.VMEM((2, 2, half, side), F32),
            pltpu.VMEM((2, 2, half, half), F32),
            pltpu.VMEM((2, side, side), BF),
            pltpu.VMEM((2, side, side), BF),
            pltpu.VMEM((2, side, side), BF),
            pltpu.VMEM((steps, side, side), BF),
            pltpu.VMEM((steps, side, side), BF),
            pltpu.SemaphoreType.DMA,
        ],
        compiler_params=pltpu.CompilerParams(vmem_limit_bytes=LIMIT),
    )(slots, layers, scales, got)


def unpack_body(places, got, update, ordered, sem):
    blocks = got.shape[0]
    chunk = blocks // CHUNKS
    stores = []
    for c in range(CHUNKS):

        def place(j, carry):
            ordered[j] = got[places[j]]
            return carry

        lax.fori_loop(c * chunk, (c + 1) * chunk, place, 0, unroll=16)
        span = pl.ds(c * chunk, chunk)
        stores.append(pltpu.make_async_copy(ordered.at[span], update.at[span], sem.at[c]))
        stores[c].start()
    for store in stores:
        store.wait()


def unpack(places, got):
    return pl.pallas_call(
        unpack_body,
        out_shape=jax.ShapeDtypeStruct(got.shape, got.dtype),
        in_specs=[
            pl.BlockSpec(memory_space=pltpu.SMEM),
            pl.BlockSpec(memory_space=pltpu.VMEM),
        ],
        out_specs=pl.BlockSpec(memory_space=pl.ANY),
        scratch_shapes=[pltpu.VMEM(got.shape, got.dtype), pltpu.SemaphoreType.DMA((CHUNKS,))],
        compiler_params=pltpu.CompilerParams(vmem_limit_bytes=LIMIT),
    )(places, got)


def in_hbm(x):
    return pltpu.with_memory_space_constraint(x, pltpu.HBM)


def body(gradients, factors, slot_block, layer_of_block, layer_step_scale):
    axes = ("row", "col")
    tables = (slot_block, layer_of_block, layer_step_scale)
    slot_block, layer_of_block, layer_step_scale = map(in_hbm, tables)
    gradients = in_hbm(gradients)
    factors = in_hbm(factors)
    message, places = pack(slot_block, gradients, factors)
    owned = lax.all_to_all(message, axes, split_axis=0, concat_axis=0, tiled=True)
    owned = pltpu.with_memory_space_constraint(owned, pltpu.VMEM)
    new_factors, moved = compute(
        slot_block, layer_of_block, layer_step_scale, owned, gradients.shape[0]
    )
    returned = lax.all_to_all(moved, axes, split_axis=0, concat_axis=0, tiled=True)
    returned = pltpu.with_memory_space_constraint(returned, pltpu.VMEM)
    return (new_factors, unpack(places, returned))


def solution(mesh):
    return jax.shard_map(
        body,
        mesh=mesh,
        in_specs=(
            P(None, None, ("row", "col"), None),
            P(None, None, ("row", "col"), None),
            P(),
            P(),
            P(),
        ),
        out_specs=(P(None, ("row", "col"), None, None), P(None, ("row", "col"), None)),
        check_vma=False,
    )
```

```python
import jax
import jax.numpy as jnp
from jax import lax
from jax.experimental import pallas as pl
from jax.experimental.pallas import tpu as pltpu
from jax.sharding import PartitionSpec as P

ITERS = 6
TILE = 128
CHUNKS = 4
LIMIT = 32 * 1024 * 1024
BF = jnp.bfloat16
F32 = jnp.float32


def pack_body(
    slots_hbm, grads, factors, msg, places, slots, g_in, f_in, sem_s, sem_g, sem_f
):
    steps, blocks, rows, side = grads.shape
    wide = steps * side
    tiles = side // TILE
    table = pltpu.make_async_copy(slots_hbm, slots, sem_s)
    table.start()
    band = lax.axis_index("row")
    odd = lax.rem(band, 2)
    picks = (2 * odd, 1, 2 - 2 * odd)
    tile_loads = []
    for f in range(2):
        for t, pick in enumerate(picks):
            start = pl.multiple_of(lax.rem(band // 2 + pick, tiles) * TILE, TILE)
            tile = factors.at[f, :, :, pl.ds(start, TILE)]
            tile_loads.append(pltpu.make_async_copy(tile, f_in.at[f, t], sem_f.at[f, t]))
    loads = [pltpu.make_async_copy(grads.at[s], g_in.at[s], sem_g.at[s]) for s in range(steps)]
    for load in loads + tile_loads:
        load.start()
    table.wait()

    def invert(j, carry):
        places[slots[j]] = j
        return carry

    lax.fori_loop(0, blocks, invert, 0, unroll=16)
    for s in range(steps):
        loads[s].wait()

        def gather(j, carry):
            msg[j, :, pl.ds(s * side, side)] = g_in[s, slots[j]]
            return carry

        lax.fori_loop(0, blocks, gather, 0, unroll=64)
    for load in tile_loads:
        load.wait()
    lane = lax.broadcasted_iota(jnp.int32, (rows, TILE), 1)
    mine = (lane // (TILE // 2)) == odd

    def convert(j, carry):
        block = slots[j]
        for f in range(2):
            for t in range(2):
                lo = wide + (2 * f + t) * TILE
                msg[j, :, pl.ds(lo, TILE)] = f_in[f, t, block].astype(BF)
        other = pltpu.roll(f_in[1, 2, block], TILE // 2, 1)
        shared = jnp.where(mine, f_in[0, 2, block], other)
        msg[j, :, pl.ds(wide + 4 * TILE, TILE)] = shared.astype(BF)
        return carry

    lax.fori_loop(0, blocks, convert, 0, unroll=128)


def pack(slots, grads, factors):
    steps, blocks, rows, side = grads.shape
    shape = (blocks, rows, steps * side + 5 * TILE)
    anywhere = pl.BlockSpec(memory_space=pl.ANY)
    return pl.pallas_call(
        pack_body,
        out_shape=(
            pltpu.VMEM(shape, BF),
            jax.ShapeDtypeStruct(slots.shape, jnp.int32),
        ),
        in_specs=[anywhere, anywhere, anywhere],
        out_specs=(
            pl.BlockSpec(memory_space=pltpu.VMEM),
            pl.BlockSpec(memory_space=pltpu.SMEM),
        ),
        scratch_shapes=[
            pltpu.SMEM(slots.shape, jnp.int32),
            pltpu.VMEM(grads.shape, BF),
            pltpu.VMEM((2, 3, blocks, rows, TILE), F32),
            pltpu.SemaphoreType.DMA,
            pltpu.SemaphoreType.DMA((steps,)),
            pltpu.SemaphoreType.DMA((2, 3)),
        ],
        compiler_params=pltpu.CompilerParams(vmem_limit_bytes=LIMIT),
    )(slots, grads, factors)


def mm(a, b):
    return jnp.dot(a, b, preferred_element_type=F32)


def put(ref, f, top, low):
    half = low.shape[0]
    ref[f, :half, :] = top
    ref[f, half:, :half] = top[:, half:].T
    ref[f, half:, half:] = low


def symmetric_product(a_ref, b_ref, f):
    half = a_ref.shape[1] // 2
    right = mm(a_ref[f], b_ref[f, :, half:])
    left = mm(a_ref[f, :half, :], b_ref[f, :, :half])
    return jnp.concatenate([left, right[:half]], axis=1), right[half:]


def compute_body(
    slots, layers, scales, got, stats, update,
    stat_ref, top_ref, low_ref, m_ref, x_ref, w_ref, g_ref, t_ref, sem,
):
    sources, rows, _ = got.shape
    side = sources * rows
    half = side // 2
    tiles = side // TILE
    per = sources // tiles
    steps = g_ref.shape[0]
    mid = tiles // 2

    band = per // 2
    base = steps * side

    def rows_of(i, parity, lo):
        first = i * per + parity * band
        piece = got[first : first + band, :, base + lo : base + lo + TILE]
        return piece.reshape(TILE // 2, TILE).astype(F32)

    def halves(f, i, parity):
        piece = rows_of(i, parity, 4 * TILE)
        return pltpu.roll(piece, TILE // 2, 1) if f else piece

    def own(f, i, parity, t):
        return rows_of(i, parity, (2 * f + t) * TILE)

    def near(f, i):
        return jnp.concatenate([own(f, i, 0, 0), halves(f, i, 1)], axis=0)

    def next_to(f, i):
        return jnp.concatenate([own(f, i, 0, 1), own(f, i, 1, 1)], axis=0)

    def far(f, i):
        return jnp.concatenate([halves(f, i, 0), own(f, i, 1, 0)], axis=0)

    upper_row = lax.broadcasted_iota(jnp.int32, (TILE, TILE), 0) < TILE // 2
    upper_col = lax.broadcasted_iota(jnp.int32, (TILE, TILE), 1) < TILE // 2

    def block(f, i, k):
        t = (k - i) % tiles
        if t == 0:
            piece = near(f, i)
            return jnp.where(jnp.logical_or(upper_row, ~upper_col), piece, piece.T)
        if t == 1:
            return next_to(f, i)
        if t == 2:
            return jnp.where(jnp.logical_or(~upper_row, upper_col), far(f, i), far(f, k).T)
        return next_to(f, k).T

    for s in range(steps):
        g_ref[s] = got[:, :, s * side : (s + 1) * side].reshape(side, side)
        t_ref[s] = g_ref[s].T
    for f, (left, right) in enumerate(((g_ref, t_ref), (t_ref, g_ref))):
        parts = [symmetric_product(left, right, s) for s in range(steps)]
        top = sum(part[0] for part in parts[1:]) + parts[0][0]
        low = sum(part[1] for part in parts[1:]) + parts[0][1]
        for i in range(tiles):
            for k in range(tiles):
                if i >= mid and k < mid:
                    continue
                piece = block(f, i, k)
                a = slice(i * TILE, (i + 1) * TILE)
                c = slice(k * TILE, (k + 1) * TILE)
                if i < mid:
                    gram = top[a, c]
                else:
                    gram = low[(i - mid) * TILE : (i - mid + 1) * TILE, (k - mid) * TILE : (k - mid + 1) * TILE]
                stat_ref[f, 0, a, c] = gram * (1.0 / side) + piece
        put(m_ref, f, stat_ref[f, 0, :half, :].astype(BF), stat_ref[f, 0, half:, half:].astype(BF))
        stat_ref[f, 0, half:, :half] = stat_ref[f, 0, :half, half:].T
    out = pltpu.make_async_copy(stat_ref, stats, sem)
    out.start()
    eye = (
        lax.broadcasted_iota(jnp.int32, (half, half), 0)
        == lax.broadcasted_iota(jnp.int32, (half, half), 1)
    )
    unit = jnp.where(eye, 1.25, 0.0)
    wide_unit = jnp.concatenate([unit, jnp.zeros((half, half), F32)], axis=1)

    def total(x):
        return jnp.sum(jnp.sum(x * x, axis=0, keepdims=True), axis=1, keepdims=True)

    inverse = []
    for f in range(2):
        top = stat_ref[f, 0, :half, :]
        low = stat_ref[f, 0, half:, half:]
        norm = jnp.sqrt(total(top) + total(top[:, half:]) + total(low))
        inverse.append((1.0 / norm, lax.rsqrt(jnp.sqrt(norm))))
    for f in range(2):
        inv = inverse[f][0]
        top, low = symmetric_product(m_ref, m_ref, f)
        top = (0.0625 * top * inv - 0.625 * stat_ref[f, 0, :half, :]) * inv
        low = (0.0625 * low * inv - 0.625 * stat_ref[f, 0, half:, half:]) * inv
        put(w_ref, f, top.astype(BF), low.astype(BF))
    for f in range(2):
        inv, first = inverse[f]
        stat_top = stat_ref[f, 0, :half, :]
        stat_low = stat_ref[f, 0, half:, half:]
        top, low = symmetric_product(w_ref, m_ref, f)
        top = (1.5625 * stat_top + top) * inv
        low = (1.5625 * stat_low + low) * inv
        top_ref[0, f] = top
        low_ref[0, f] = low
        put(m_ref, f, top.astype(BF), low.astype(BF))
        top = first * (wide_unit - (0.25 * inv) * stat_top)
        low = first * (unit - (0.25 * inv) * stat_low)
        top_ref[1, f] = top
        low_ref[1, f] = low
        put(x_ref, f, top.astype(BF), low.astype(BF))

    def last_m():
        for f in range(2):
            top, low = symmetric_product(w_ref, m_ref, f)
            top = 1.5625 * top_ref[0, f] + top
            low = 1.5625 * low_ref[0, f] + low
            top_ref[0, f] = top
            low_ref[0, f] = low
            put(m_ref, f, top.astype(BF), low.astype(BF))

    last_m()

    def move_x(f):
        top, low = symmetric_product(x_ref, m_ref, f)
        top = 1.25 * top_ref[1, f] - 0.25 * top
        low = 1.25 * low_ref[1, f] - 0.25 * low
        top_ref[1, f] = top
        low_ref[1, f] = low
        put(x_ref, f, top.astype(BF), low.astype(BF))

    def move_m():
        for f in range(2):
            top, low = symmetric_product(m_ref, m_ref, f)
            top = 0.0625 * top - 0.625 * top_ref[0, f]
            low = 0.0625 * low - 0.625 * low_ref[0, f]
            put(w_ref, f, top.astype(BF), low.astype(BF))
        last_m()
        last_m()

    def sweep(k, carry):
        for f in range(2):
            move_x(f)
        move_m()
        return carry

    lax.fori_loop(1, ITERS - 1, sweep, 0)
    for f in range(2):
        move_x(f)
    me = lax.axis_index("row") * lax.axis_size("col") + lax.axis_index("col")
    scale = scales[layers[slots[me]]]
    applied = mm(x_ref[0], g_ref[steps - 1]).astype(BF)
    result = (scale * mm(applied, x_ref[1])).astype(BF)
    update[...] = result.reshape(sources, rows, side)
    out.wait()


def compute(slots, layers, scales, got, steps):
    sources, rows, _ = got.shape
    side = sources * rows
    half = side // 2
    smem = pl.BlockSpec(memory_space=pltpu.SMEM)
    return pl.pallas_call(
        compute_body,
        out_shape=(
            jax.ShapeDtypeStruct((2, 1, side, side), F32),
            pltpu.VMEM((sources, rows, side), BF),
        ),
        in_specs=[smem, smem, smem, pl.BlockSpec(memory_space=pltpu.VMEM)],
        out_specs=(
            pl.BlockSpec(memory_space=pl.ANY),
            pl.BlockSpec(memory_space=pltpu.VMEM),
        ),
        scratch_shapes=[
            pltpu.VMEM((2, 1, side, side), F32),
            pltpu.VMEM((2, 2, half, side), F32),
            pltpu.VMEM((2, 2, half, half), F32),
            pltpu.VMEM((2, side, side), BF),
            pltpu.VMEM((2, side, side), BF),
            pltpu.VMEM((2, side, side), BF),
            pltpu.VMEM((steps, side, side), BF),
            pltpu.VMEM((steps, side, side), BF),
            pltpu.SemaphoreType.DMA,
        ],
        compiler_params=pltpu.CompilerParams(vmem_limit_bytes=LIMIT),
    )(slots, layers, scales, got)


def unpack_body(places, got, update, ordered, sem):
    blocks = got.shape[0]
    chunk = blocks // CHUNKS
    stores = []
    for c in range(CHUNKS):

        def place(j, carry):
            ordered[j] = got[places[j]]
            return carry

        lax.fori_loop(c * chunk, (c + 1) * chunk, place, 0, unroll=32)
        span = pl.ds(c * chunk, chunk)
        stores.append(pltpu.make_async_copy(ordered.at[span], update.at[span], sem.at[c]))
        stores[c].start()
    for store in stores:
        store.wait()


def unpack(places, got):
    return pl.pallas_call(
        unpack_body,
        out_shape=jax.ShapeDtypeStruct(got.shape, got.dtype),
        in_specs=[
            pl.BlockSpec(memory_space=pltpu.SMEM),
            pl.BlockSpec(memory_space=pltpu.VMEM),
        ],
        out_specs=pl.BlockSpec(memory_space=pl.ANY),
        scratch_shapes=[pltpu.VMEM(got.shape, got.dtype), pltpu.SemaphoreType.DMA((CHUNKS,))],
        compiler_params=pltpu.CompilerParams(vmem_limit_bytes=LIMIT),
    )(places, got)


def in_hbm(x):
    return pltpu.with_memory_space_constraint(x, pltpu.HBM)


def body(gradients, factors, slot_block, layer_of_block, layer_step_scale):
    axes = ("row", "col")
    tables = (slot_block, layer_of_block, layer_step_scale)
    slot_block, layer_of_block, layer_step_scale = map(in_hbm, tables)
    gradients = in_hbm(gradients)
    factors = in_hbm(factors)
    message, places = pack(slot_block, gradients, factors)
    owned = lax.all_to_all(message, axes, split_axis=0, concat_axis=0, tiled=True)
    owned = pltpu.with_memory_space_constraint(owned, pltpu.VMEM)
    new_factors, moved = compute(
        slot_block, layer_of_block, layer_step_scale, owned, gradients.shape[0]
    )
    returned = lax.all_to_all(moved, axes, split_axis=0, concat_axis=0, tiled=True)
    returned = pltpu.with_memory_space_constraint(returned, pltpu.VMEM)
    return (new_factors, unpack(places, returned))


def solution(mesh):
    return jax.shard_map(
        body,
        mesh=mesh,
        in_specs=(
            P(None, None, ("row", "col"), None),
            P(None, None, ("row", "col"), None),
            P(),
            P(),
            P(),
        ),
        out_specs=(P(None, ("row", "col"), None, None), P(None, ("row", "col"), None)),
        check_vma=False,
    )
```

```python
import jax
import jax.numpy as jnp
from jax import lax
from jax.experimental import pallas as pl
from jax.experimental.pallas import tpu as pltpu
from jax.sharding import PartitionSpec as P

ITERS = 6
TILE = 128
CHUNKS = 4
LIMIT = 32 * 1024 * 1024
BF = jnp.bfloat16
F32 = jnp.float32


def pack_body(
    slots_hbm, grads, factors, msg, places, slots, g_in, f_in, sem_s, sem_g, sem_f
):
    steps, blocks, rows, side = grads.shape
    wide = steps * side
    tiles = side // TILE
    table = pltpu.make_async_copy(slots_hbm, slots, sem_s)
    table.start()
    band = lax.axis_index("row")
    odd = lax.rem(band, 2)
    picks = (2 * odd, 1, 2 - 2 * odd)
    tile_loads = []
    for f in range(2):
        for t, pick in enumerate(picks):
            start = pl.multiple_of(lax.rem(band // 2 + pick, tiles) * TILE, TILE)
            tile = factors.at[f, :, :, pl.ds(start, TILE)]
            tile_loads.append(pltpu.make_async_copy(tile, f_in.at[f, t], sem_f.at[f, t]))
    loads = [pltpu.make_async_copy(grads.at[s], g_in.at[s], sem_g.at[s]) for s in range(steps)]
    for load in loads + tile_loads:
        load.start()
    table.wait()

    def invert(j, carry):
        places[slots[j]] = j
        return carry

    lax.fori_loop(0, blocks, invert, 0, unroll=16)
    for s in range(steps):
        loads[s].wait()

        def gather(j, carry):
            msg[j, :, pl.ds(s * side, side)] = g_in[s, slots[j]]
            return carry

        lax.fori_loop(0, blocks, gather, 0, unroll=64)
    lane = lax.broadcasted_iota(jnp.int32, (rows, TILE), 1)
    mine = (lane // (TILE // 2)) == odd
    for f in range(2):
        for load in tile_loads[3 * f : 3 * f + 3]:
            load.wait()

        def convert(j, carry):
            block = slots[j]
            for t in range(2):
                lo = wide + (2 * f + t) * TILE
                msg[j, :, pl.ds(lo, TILE)] = f_in[f, t, block].astype(BF)
            if f:
                other = pltpu.roll(f_in[1, 2, block], TILE // 2, 1)
                shared = jnp.where(mine, f_in[0, 2, block], other)
                msg[j, :, pl.ds(wide + 4 * TILE, TILE)] = shared.astype(BF)
            return carry

        lax.fori_loop(0, blocks, convert, 0, unroll=128)


def pack(slots, grads, factors):
    steps, blocks, rows, side = grads.shape
    shape = (blocks, rows, steps * side + 5 * TILE)
    anywhere = pl.BlockSpec(memory_space=pl.ANY)
    return pl.pallas_call(
        pack_body,
        out_shape=(
            pltpu.VMEM(shape, BF),
            jax.ShapeDtypeStruct(slots.shape, jnp.int32),
        ),
        in_specs=[anywhere, anywhere, anywhere],
        out_specs=(
            pl.BlockSpec(memory_space=pltpu.VMEM),
            pl.BlockSpec(memory_space=pltpu.SMEM),
        ),
        scratch_shapes=[
            pltpu.SMEM(slots.shape, jnp.int32),
            pltpu.VMEM(grads.shape, BF),
            pltpu.VMEM((2, 3, blocks, rows, TILE), F32),
            pltpu.SemaphoreType.DMA,
            pltpu.SemaphoreType.DMA((steps,)),
            pltpu.SemaphoreType.DMA((2, 3)),
        ],
        compiler_params=pltpu.CompilerParams(vmem_limit_bytes=LIMIT),
    )(slots, grads, factors)


def mm(a, b):
    return jnp.dot(a, b, preferred_element_type=F32)


def put(ref, f, top, low):
    half = low.shape[0]
    ref[f, :half, :] = top
    ref[f, half:, :half] = top[:, half:].T
    ref[f, half:, half:] = low


def symmetric_product(a_ref, b_ref, f):
    half = a_ref.shape[1] // 2
    right = mm(a_ref[f], b_ref[f, :, half:])
    left = mm(a_ref[f, :half, :], b_ref[f, :, :half])
    return jnp.concatenate([left, right[:half]], axis=1), right[half:]


def compute_body(
    slots, layers, scales, got, stats, update,
    stat_ref, top_ref, low_ref, m_ref, x_ref, w_ref, g_ref, t_ref, sem,
):
    sources, rows, _ = got.shape
    side = sources * rows
    half = side // 2
    tiles = side // TILE
    per = sources // tiles
    steps = g_ref.shape[0]
    mid = tiles // 2

    band = per // 2
    base = steps * side

    def rows_of(i, parity, lo):
        first = i * per + parity * band
        piece = got[first : first + band, :, base + lo : base + lo + TILE]
        return piece.reshape(TILE // 2, TILE).astype(F32)

    def halves(f, i, parity):
        piece = rows_of(i, parity, 4 * TILE)
        return pltpu.roll(piece, TILE // 2, 1) if f else piece

    def own(f, i, parity, t):
        return rows_of(i, parity, (2 * f + t) * TILE)

    def near(f, i):
        return jnp.concatenate([own(f, i, 0, 0), halves(f, i, 1)], axis=0)

    def next_to(f, i):
        return jnp.concatenate([own(f, i, 0, 1), own(f, i, 1, 1)], axis=0)

    def far(f, i):
        return jnp.concatenate([halves(f, i, 0), own(f, i, 1, 0)], axis=0)

    upper_row = lax.broadcasted_iota(jnp.int32, (TILE, TILE), 0) < TILE // 2
    upper_col = lax.broadcasted_iota(jnp.int32, (TILE, TILE), 1) < TILE // 2

    def block(f, i, k):
        t = (k - i) % tiles
        if t == 0:
            piece = near(f, i)
            return jnp.where(jnp.logical_or(upper_row, ~upper_col), piece, piece.T)
        if t == 1:
            return next_to(f, i)
        if t == 2:
            return jnp.where(jnp.logical_or(~upper_row, upper_col), far(f, i), far(f, k).T)
        return next_to(f, k).T

    for s in range(steps):
        g_ref[s] = got[:, :, s * side : (s + 1) * side].reshape(side, side)
        t_ref[s] = g_ref[s].T
    for f, (left, right) in enumerate(((g_ref, t_ref), (t_ref, g_ref))):
        parts = [symmetric_product(left, right, s) for s in range(steps)]
        top = sum(part[0] for part in parts[1:]) + parts[0][0]
        low = sum(part[1] for part in parts[1:]) + parts[0][1]
        for i in range(tiles):
            for k in range(tiles):
                if i >= mid and k < mid:
                    continue
                piece = block(f, i, k)
                a = slice(i * TILE, (i + 1) * TILE)
                c = slice(k * TILE, (k + 1) * TILE)
                if i < mid:
                    gram = top[a, c]
                else:
                    gram = low[(i - mid) * TILE : (i - mid + 1) * TILE, (k - mid) * TILE : (k - mid + 1) * TILE]
                stat_ref[f, 0, a, c] = gram * (1.0 / side) + piece
        put(m_ref, f, stat_ref[f, 0, :half, :].astype(BF), stat_ref[f, 0, half:, half:].astype(BF))
        stat_ref[f, 0, half:, :half] = stat_ref[f, 0, :half, half:].T
    out = pltpu.make_async_copy(stat_ref, stats, sem)
    out.start()
    eye = (
        lax.broadcasted_iota(jnp.int32, (half, half), 0)
        == lax.broadcasted_iota(jnp.int32, (half, half), 1)
    )
    unit = jnp.where(eye, 1.25, 0.0)
    wide_unit = jnp.concatenate([unit, jnp.zeros((half, half), F32)], axis=1)

    def total(x):
        return jnp.sum(jnp.sum(x * x, axis=0, keepdims=True), axis=1, keepdims=True)

    inverse = []
    for f in range(2):
        top = stat_ref[f, 0, :half, :]
        low = stat_ref[f, 0, half:, half:]
        norm = jnp.sqrt(total(top) + total(top[:, half:]) + total(low))
        inverse.append((1.0 / norm, lax.rsqrt(jnp.sqrt(norm))))
    for f in range(2):
        inv = inverse[f][0]
        top, low = symmetric_product(m_ref, m_ref, f)
        top = (0.0625 * top * inv - 0.625 * stat_ref[f, 0, :half, :]) * inv
        low = (0.0625 * low * inv - 0.625 * stat_ref[f, 0, half:, half:]) * inv
        put(w_ref, f, top.astype(BF), low.astype(BF))
    for f in range(2):
        inv, first = inverse[f]
        stat_top = stat_ref[f, 0, :half, :]
        stat_low = stat_ref[f, 0, half:, half:]
        top, low = symmetric_product(w_ref, m_ref, f)
        top = (1.5625 * stat_top + top) * inv
        low = (1.5625 * stat_low + low) * inv
        top_ref[0, f] = top
        low_ref[0, f] = low
        put(m_ref, f, top.astype(BF), low.astype(BF))
        top = first * (wide_unit - (0.25 * inv) * stat_top)
        low = first * (unit - (0.25 * inv) * stat_low)
        top_ref[1, f] = top
        low_ref[1, f] = low
        put(x_ref, f, top.astype(BF), low.astype(BF))

    def last_m():
        for f in range(2):
            top, low = symmetric_product(w_ref, m_ref, f)
            top = 1.5625 * top_ref[0, f] + top
            low = 1.5625 * low_ref[0, f] + low
            top_ref[0, f] = top
            low_ref[0, f] = low
            put(m_ref, f, top.astype(BF), low.astype(BF))

    last_m()

    def move_x(f):
        top, low = symmetric_product(x_ref, m_ref, f)
        top = 1.25 * top_ref[1, f] - 0.25 * top
        low = 1.25 * low_ref[1, f] - 0.25 * low
        top_ref[1, f] = top
        low_ref[1, f] = low
        put(x_ref, f, top.astype(BF), low.astype(BF))

    def move_m():
        for f in range(2):
            top, low = symmetric_product(m_ref, m_ref, f)
            top = 0.0625 * top - 0.625 * top_ref[0, f]
            low = 0.0625 * low - 0.625 * low_ref[0, f]
            put(w_ref, f, top.astype(BF), low.astype(BF))
        last_m()
        last_m()

    def sweep(k, carry):
        for f in range(2):
            move_x(f)
        move_m()
        return carry

    lax.fori_loop(1, ITERS - 1, sweep, 0)
    for f in range(2):
        move_x(f)
    me = lax.axis_index("row") * lax.axis_size("col") + lax.axis_index("col")
    scale = scales[layers[slots[me]]]
    applied = mm(x_ref[0], g_ref[steps - 1]).astype(BF)
    result = (scale * mm(applied, x_ref[1])).astype(BF)
    update[...] = result.reshape(sources, rows, side)
    out.wait()


def compute(slots, layers, scales, got, steps):
    sources, rows, _ = got.shape
    side = sources * rows
    half = side // 2
    smem = pl.BlockSpec(memory_space=pltpu.SMEM)
    return pl.pallas_call(
        compute_body,
        out_shape=(
            jax.ShapeDtypeStruct((2, 1, side, side), F32),
            pltpu.VMEM((sources, rows, side), BF),
        ),
        in_specs=[smem, smem, smem, pl.BlockSpec(memory_space=pltpu.VMEM)],
        out_specs=(
            pl.BlockSpec(memory_space=pl.ANY),
            pl.BlockSpec(memory_space=pltpu.VMEM),
        ),
        scratch_shapes=[
            pltpu.VMEM((2, 1, side, side), F32),
            pltpu.VMEM((2, 2, half, side), F32),
            pltpu.VMEM((2, 2, half, half), F32),
            pltpu.VMEM((2, side, side), BF),
            pltpu.VMEM((2, side, side), BF),
            pltpu.VMEM((2, side, side), BF),
            pltpu.VMEM((steps, side, side), BF),
            pltpu.VMEM((steps, side, side), BF),
            pltpu.SemaphoreType.DMA,
        ],
        compiler_params=pltpu.CompilerParams(vmem_limit_bytes=LIMIT),
    )(slots, layers, scales, got)


def unpack_body(places, got, update, ordered, sem):
    blocks = got.shape[0]
    chunk = blocks // CHUNKS
    stores = []
    for c in range(CHUNKS):

        def place(j, carry):
            ordered[j] = got[places[j]]
            return carry

        lax.fori_loop(c * chunk, (c + 1) * chunk, place, 0, unroll=32)
        span = pl.ds(c * chunk, chunk)
        stores.append(pltpu.make_async_copy(ordered.at[span], update.at[span], sem.at[c]))
        stores[c].start()
    for store in stores:
        store.wait()


def unpack(places, got):
    return pl.pallas_call(
        unpack_body,
        out_shape=jax.ShapeDtypeStruct(got.shape, got.dtype),
        in_specs=[
            pl.BlockSpec(memory_space=pltpu.SMEM),
            pl.BlockSpec(memory_space=pltpu.VMEM),
        ],
        out_specs=pl.BlockSpec(memory_space=pl.ANY),
        scratch_shapes=[pltpu.VMEM(got.shape, got.dtype), pltpu.SemaphoreType.DMA((CHUNKS,))],
        compiler_params=pltpu.CompilerParams(vmem_limit_bytes=LIMIT),
    )(places, got)


def in_hbm(x):
    return pltpu.with_memory_space_constraint(x, pltpu.HBM)


def body(gradients, factors, slot_block, layer_of_block, layer_step_scale):
    axes = ("row", "col")
    tables = (slot_block, layer_of_block, layer_step_scale)
    slot_block, layer_of_block, layer_step_scale = map(in_hbm, tables)
    gradients = in_hbm(gradients)
    factors = in_hbm(factors)
    message, places = pack(slot_block, gradients, factors)
    owned = lax.all_to_all(message, axes, split_axis=0, concat_axis=0, tiled=True)
    owned = pltpu.with_memory_space_constraint(owned, pltpu.VMEM)
    new_factors, moved = compute(
        slot_block, layer_of_block, layer_step_scale, owned, gradients.shape[0]
    )
    returned = lax.all_to_all(moved, axes, split_axis=0, concat_axis=0, tiled=True)
    returned = pltpu.with_memory_space_constraint(returned, pltpu.VMEM)
    return (new_factors, unpack(places, returned))


def solution(mesh):
    return jax.shard_map(
        body,
        mesh=mesh,
        in_specs=(
            P(None, None, ("row", "col"), None),
            P(None, None, ("row", "col"), None),
            P(),
            P(),
            P(),
        ),
        out_specs=(P(None, ("row", "col"), None, None), P(None, ("row", "col"), None)),
        check_vma=False,
    )
```
